256 devices in a mesh: slides: 4 (over y, x), rows: 32 (over z), cols: 2 (over core).
Axes of the slice: x: 2, y: 2, z: 32, core: 2. Of those that a mesh axis runs over, the one named last changes fastest.
The devices are a block of a 4x8x32 slice.
Arguments:
- image: bfloat16 [4096, 512, 128], P(('slides', 'rows'), 'cols'), parts along dimension 0, may hold values from -6 to 6
- tissue: int32 [128, 16], P(('slides', 'rows'), 'cols'), parts along dimension 0, may hold values 0 or 1
- first_kernel: bfloat16 [3, 3, 128, 128], replicated, may hold values from -0.1875 to 0.1875
- first_bias: float32 [128], replicated, may hold values from -3 to 3
- second_kernel: bfloat16 [3, 3, 128, 128], replicated, may hold values from -0.1875 to 0.1875
- second_bias: float32 [128], replicated, may hold values from -3 to 3
Outputs:
- features: bfloat16 [4096, 512, 128], P(('slides', 'rows'), 'cols'), parts along dimension 0
The draws below stay inside these ranges and needn't reach their ends.
There are 4 independent parts, one for each index of `slides`. The reference program is written for one: setup_inputs(seed, part) draws one part's arguments, and reference() takes and returns one part's arrays. A program takes and returns all parts, laid end to end along the dimension named above; an argument that names none is the same for every part. Nothing has to cross between parts.
All inputs are finite; a program needn't handle non-finite values. No bound on the sum of `tissue` on one device may be relied on, other than what follows from the above.
Results may differ from the reference program's by a relative error of at most 0.0043.
Values may be sent and summed in bfloat16 or wider, within the bound.
A program may use at most 128 MiB of HBM per device.

```python
import jax
import jax.numpy as jnp

C = 128
MB = 32
H = 1024
W = 512


def place_ends(array, own_key, least, high):
    longest = array.shape.index(max(array.shape))
    spots = []
    for shift in (0, 1):
        where = [jax.random.randint(jax.random.fold_in(own_key, axis), (), 0, length) for axis, length in enumerate(array.shape)]
        where[longest] = (where[longest] + shift) % array.shape[longest]
        spots.append(tuple(where))
    return array.at[spots[0]].set(least).at[spots[1]].set(high)


def block_scale(own_key, shape, shards, low, top_value):
    loudness, own = 1.0, jax.random.fold_in(own_key, 6)
    for position, parts in shards:
        steps = jnp.exp(jax.random.uniform(jax.random.fold_in(own, position), (parts,), jnp.float32, low / len(shards), top_value / len(shards)))
        loudness = loudness * jnp.repeat(steps, shape[position] // parts).reshape([-1 if axis == position else 1 for axis in range(len(shape))])
    return loudness


def normal_values(stream_key, dims, spread, bound, pieces=(), kind=jnp.bfloat16):
    entries = jax.random.normal(stream_key, dims, jnp.float32) * spread
    if len(pieces) > 0:
        entries = block_scale(stream_key, dims, pieces, -0.22, 0.18) * entries
    return jnp.clip(entries, min=-bound, max=bound).astype(kind)


def setup_inputs(seed: int = 0, part: int = 0) -> dict:
    keys = jax.random.split(jax.random.key(seed), 7)
    part_keys = jax.random.split(jax.random.fold_in(keys[6], part), 7)
    return {
        "image": normal_values(part_keys[0], (H, W, C), 1.0, 6.0, ((0, 32), (1, 2))),
        "tissue": place_ends((jax.random.randint(part_keys[1], (H // MB, W // MB), 0, 5) < 3).astype(jnp.int32), jax.random.fold_in(part_keys[1], 1), 0, 1),
        "first_kernel": normal_values(keys[2], (3, 3, C, C), (9 * C) ** -0.5, 0.1875),
        "first_bias": normal_values(keys[3], (C,), 0.5, 3.0, (), jnp.float32),
        "second_kernel": normal_values(keys[4], (3, 3, C, C), (9 * C) ** -0.5, 0.1875),
        "second_bias": normal_values(keys[5], (C,), 0.5, 3.0, (), jnp.float32),
    }


def conv_valid(padded, kernel, bias):
    rows = padded.shape[0] - 2
    cols = padded.shape[1] - 2
    chans = padded.shape[2]
    wide = jnp.concatenate([padded[:, 0:cols], padded[:, 1:cols + 1], padded[:, 2:cols + 2]], axis=-1)
    total = jnp.zeros((rows * cols, kernel.shape[3]), jnp.float32)
    for offset in range(3):
        block = wide[offset:offset + rows].reshape(rows * cols, 3 * chans)
        total = total + jnp.dot(block, kernel[offset].reshape(3 * chans, kernel.shape[3]), preferred_element_type=jnp.float32)
    return total.reshape(rows, cols, kernel.shape[3]) + bias


def reference(image, tissue, first_kernel, first_bias, second_kernel, second_bias):
    pixel_mask = jnp.repeat(jnp.repeat(tissue, MB, axis=0), MB, axis=1).astype(jnp.float32)[:, :, None]
    padded = jnp.pad(image, ((1, 1), (1, 1), (0, 0)))
    hidden = (jnp.maximum(conv_valid(padded, first_kernel, first_bias), 0.0) * pixel_mask).astype(jnp.bfloat16)
    padded = jnp.pad(hidden, ((1, 1), (1, 1), (0, 0)))
    return (jnp.maximum(conv_valid(padded, second_kernel, second_bias), 0.0) * pixel_mask).astype(jnp.bfloat16)
```

```python
import functools

import jax
import jax.numpy as jnp
from jax import lax
from jax.experimental import pallas as pl
from jax.experimental.pallas import tpu as pltpu
from jax.sharding import PartitionSpec as P

MESH = pl.DeviceIdType.MESH
MB = 32
BF = jnp.bfloat16
F32 = jnp.float32
UP, DOWN, SIDE, DUP, DDN = range(5)


def kernel(
    image, tissue, k1, b1, k2, b2, out,
    xr, xm, xp, pb, col, sm, s0, sp, h0, hm, hp, hs, w1, w2, bs, ts, mk, mks, fb, sf, ob,
    in_sem, out_sem, send_x, recv_x, send_t, recv_t,
):
    R, W, C = image.shape
    H = W // MB
    n = lax.axis_size("rows")
    sl, i, c = lax.axis_index("slides"), lax.axis_index("rows"), lax.axis_index("cols")
    has_up, has_down = i > 0, i < n - 1
    side0 = jnp.where(c == 0, 1.0, 0.0).astype(F32)
    side1 = 1.0 - side0
    edge = pl.multiple_of((W - 16) * (1 - c), 16)

    def load(src, dst, k):
        cp = pltpu.make_async_copy(src, dst, in_sem.at[k])
        cp.start()
        return cp

    l_top = load(image.at[0:2], xr.at[2:4], 0)
    l_bot = load(image.at[R - 2 : R], xr.at[R : R + 2], 1)
    l_col = load(image.at[:, pl.ds(edge, 16), :], col, 2)
    l_tis = load(tissue, ts.at[0], 3)
    l_w1 = [load(k1, w1.at[j * 3 * C : j * 3 * C + 9 * C, j * C : (j + 1) * C], 4 + j) for j in range(2)]
    l_img = load(image.at[2 : R - 2], xr.at[4:R], 6)
    l_b1 = load(b1, bs.at[0], 7)
    l_w2 = [load(k2, w2.at[j * 3 * C : j * 3 * C + 9 * C, j * C : (j + 1) * C], 8 + j) for j in range(2)]
    l_b2 = load(b2, bs.at[1], 10)

    up, down = (sl, i - 1, c), (sl, i + 1, c)
    dup, ddn, side = (sl, i - 1, 1 - c), (sl, i + 1, 1 - c), (sl, i, 1 - c)
    barrier = pltpu.get_barrier_semaphore()
    pl.semaphore_signal(barrier, inc=1, device_id=side, device_id_type=MESH)

    @pl.when(has_up)
    def _():
        pl.semaphore_signal(barrier, inc=1, device_id=up, device_id_type=MESH)
        pl.semaphore_signal(barrier, inc=1, device_id=dup, device_id_type=MESH)

    @pl.when(has_down)
    def _():
        pl.semaphore_signal(barrier, inc=1, device_id=down, device_id_type=MESH)
        pl.semaphore_signal(barrier, inc=1, device_id=ddn, device_id_type=MESH)

    for w in (w1, w2):
        w[9 * C : 12 * C, 0:C] = jnp.zeros((3 * C, C), BF)
        w[0 : 3 * C, C : 2 * C] = jnp.zeros((3 * C, C), BF)

    @pl.when(jnp.logical_not(has_up))
    def _():
        xr[0:2] = jnp.zeros((2, W, C), BF)
        pb[0:2] = jnp.zeros((2, 16, C), BF)
        ts[2] = jnp.zeros((1, H), jnp.int32)
        ts[4] = jnp.zeros((1, H), jnp.int32)

    @pl.when(jnp.logical_not(has_down))
    def _():
        xr[R + 2 : R + 4] = jnp.zeros((2, W, C), BF)
        pb[R + 2 : R + 4] = jnp.zeros((2, 16, C), BF)
        ts[3] = jnp.zeros((1, H), jnp.int32)
        ts[5] = jnp.zeros((1, H), jnp.int32)

    pl.semaphore_wait(barrier, 1 + 2 * has_up.astype(jnp.int32) + 2 * has_down.astype(jnp.int32))

    def remote(src, dst, sends, recvs, k, dev):
        return pltpu.make_async_remote_copy(
            src_ref=src, dst_ref=dst, send_sem=sends.at[k], recv_sem=recvs.at[k],
            device_id=dev, device_id_type=MESH,
        )

    r_up = remote(xr.at[2:4], xr.at[R + 2 : R + 4], send_x, recv_x, UP, up)
    r_down = remote(xr.at[R : R + 2], xr.at[0:2], send_x, recv_x, DOWN, down)
    r_side = remote(col, pb.at[2 : R + 2], send_x, recv_x, SIDE, side)
    r_dup = remote(col.at[0:2], pb.at[R + 2 : R + 4], send_x, recv_x, DUP, dup)
    r_ddn = remote(col.at[R - 2 : R], pb.at[0:2], send_x, recv_x, DDN, ddn)
    t_side = remote(ts.at[0], ts.at[1], send_t, recv_t, SIDE, side)
    t_down = remote(ts.at[0], ts.at[2], send_t, recv_t, DOWN, down)
    t_up = remote(ts.at[0], ts.at[3], send_t, recv_t, UP, up)
    t_ddn = remote(ts.at[0], ts.at[4], send_t, recv_t, DDN, ddn)
    t_dup = remote(ts.at[0], ts.at[5], send_t, recv_t, DUP, dup)

    l_top.wait()
    l_bot.wait()
    l_col.wait()
    l_tis.wait()
    r_side.start()
    t_side.start()

    @pl.when(has_up)
    def _():
        r_up.start()
        r_dup.start()
        t_up.start()
        t_dup.start()

    @pl.when(has_down)
    def _():
        r_down.start()
        r_ddn.start()
        t_down.start()
        t_ddn.start()

    def block_mask(slot, store):
        t = ts[slot].astype(F32)
        for j in range(H):
            mk[store, j] = jnp.broadcast_to(t[:, j : j + 1], (8, C))

    def strip_mask(slot, store):
        t = ts[slot].astype(F32)
        m = t[:, 0:1] * side0 + t[:, H - 1 : H] * side1
        mks[store] = jnp.broadcast_to(m, (8, C))

    block_mask(0, 0)
    for cp in l_w1:
        cp.wait()
    l_b1.wait()
    l_b2.wait()
    for cp in l_w2:
        cp.wait()
    l_img.wait()
    r_side.wait_recv()
    t_side.wait_recv()
    strip_mask(1, 0)

    counter = [0]

    def spread(value, left8, right8, r, center, minus, plus):
        f = fb.at[counter[0] % 4]
        counter[0] += 1
        f[0:8] = left8
        f[8 : W + 8] = value
        f[W + 8 : W + 16] = right8
        minus[r] = f[7 : W + 7].astype(BF)
        plus[r] = f[9 : W + 9].astype(BF)
        if center is not None:
            center[r] = value.astype(BF)

    def image_row(r):
        part = pb[r].astype(F32)
        own = xr[r, pl.ds(edge, 16), :].astype(F32)
        sf[r, pl.ds(pl.multiple_of(16 * c, 16), 16), :] = own
        sf[r, pl.ds(pl.multiple_of(16 * (1 - c), 16), 16), :] = part
        sm[r] = sf[r, 7:23].astype(BF)
        s0[r] = sf[r, 8:24].astype(BF)
        sp[r] = sf[r, 9:25].astype(BF)
        spread(xr[r].astype(F32), part[8:16] * side1, part[0:8] * side0, r, None, xm, xp)

    def lhs(p, refs):
        return jnp.concatenate([ref[2 * p + k] for k in range(4) for ref in refs], axis=1)

    bias1 = jnp.broadcast_to(bs[0], (8, C))
    bias2 = jnp.broadcast_to(bs[1], (8, C))

    def finish(acc, bias, store):
        z = jnp.maximum(acc.reshape(H, MB // 8, 8, C) + bias, 0.0) * mk[store][:, None]
        return z.reshape(W, C)

    def klass(r):
        return 1 if r == 0 else 2 if r == R + 1 else 0

    def strips(pairs):
        acc = jnp.dot(
            jnp.concatenate([lhs(p, (sm, s0, sp)) for p in pairs], axis=0), w1[...],
            preferred_element_type=F32,
        )
        for a, p in enumerate(pairs):
            for j in range(2):
                r = 2 * p + j
                piece = acc[a * 16 : a * 16 + 16, j * C : (j + 1) * C].reshape(2, 8, C)
                hs[r] = (jnp.maximum(piece + bias1, 0.0) * mks[klass(r)]).reshape(16, C)

    def first(pairs):
        acc = jnp.dot(
            jnp.concatenate([lhs(p, (xm, xr, xp)) for p in pairs], axis=0), w1[...],
            preferred_element_type=F32,
        )
        for a, p in enumerate(pairs):
            for j in range(2):
                r = 2 * p + j
                value = finish(acc[a * W : (a + 1) * W, j * C : (j + 1) * C], bias1, klass(r))
                side = hs[r]
                spread(value, side[0:8] * side1, side[8:16] * side0, r, h0, hm, hp)

    outs = []

    def second(pairs):
        acc = jnp.dot(
            jnp.concatenate([lhs(p, (hm, h0, hp)) for p in pairs], axis=0), w2[...],
            preferred_element_type=F32,
        )
        for a, p in enumerate(pairs):
            for j in range(2):
                ob[2 * p + j] = finish(acc[a * W : (a + 1) * W, j * C : (j + 1) * C], bias2, 0).astype(BF)

    def flush(lo, hi):
        cp = pltpu.make_async_copy(ob.at[lo:hi], out.at[lo:hi], out_sem.at[len(outs)])
        cp.start()
        outs.append(cp)

    last = R // 2
    for r in range(2, R + 2):
        image_row(r)
    strips(range(1, last))
    for p in range(1, last, 2):
        first([q for q in (p, p + 1) if q < last])
    for p in range(1, last - 1, 2):
        second([q for q in (p, p + 1) if q < last - 1])
    flush(2, R - 2)

    @pl.when(has_up)
    def _():
        r_down.wait_recv()
        r_ddn.wait_recv()
        t_down.wait_recv()
        t_ddn.wait_recv()

    @pl.when(has_down)
    def _():
        r_up.wait_recv()
        r_dup.wait_recv()
        t_up.wait_recv()
        t_dup.wait_recv()

    block_mask(2, 1)
    block_mask(3, 2)
    strip_mask(4, 1)
    strip_mask(5, 2)
    for r in (0, 1, R + 2, R + 3):
        image_row(r)
    strips((0, last))
    first((0, last))
    second((0, last - 1))
    flush(0, 2)
    flush(R - 2, R)

    r_side.wait_send()
    t_side.wait_send()

    @pl.when(has_up)
    def _():
        for cp in (r_up, r_dup, t_up, t_dup):
            cp.wait_send()

    @pl.when(has_down)
    def _():
        for cp in (r_down, r_ddn, t_down, t_ddn):
            cp.wait_send()

    for cp in outs:
        cp.wait()


def shards(image, tissue, k1, b1, k2, b2):
    R, W, C = image.shape
    H = W // MB
    any_spec = pl.BlockSpec(memory_space=pl.ANY)
    dma = pltpu.SemaphoreType.DMA
    return pl.pallas_call(
        kernel,
        out_shape=jax.ShapeDtypeStruct((R, W, C), BF),
        in_specs=[any_spec] * 6,
        out_specs=any_spec,
        scratch_shapes=[
            pltpu.VMEM((R + 4, W, C), BF),
            pltpu.VMEM((R + 4, W, C), BF),
            pltpu.VMEM((R + 4, W, C), BF),
            pltpu.VMEM((R + 4, 16, C), BF),
            pltpu.VMEM((R, 16, C), BF),
            pltpu.VMEM((R + 4, 16, C), BF),
            pltpu.VMEM((R + 4, 16, C), BF),
            pltpu.VMEM((R + 4, 16, C), BF),
            pltpu.VMEM((R + 2, W, C), BF),
            pltpu.VMEM((R + 2, W, C), BF),
            pltpu.VMEM((R + 2, W, C), BF),
            pltpu.VMEM((R + 2, 16, C), F32),
            pltpu.VMEM((12 * C, 2 * C), BF),
            pltpu.VMEM((12 * C, 2 * C), BF),
            pltpu.VMEM((2, 1, C), F32),
            pltpu.VMEM((6, 1, H), jnp.int32),
            pltpu.VMEM((3, H, 8, C), F32),
            pltpu.VMEM((3, 8, C), F32),
            pltpu.VMEM((4, W + 16, C), F32),
            pltpu.VMEM((R + 4, 32, C), F32),
            pltpu.VMEM((R, W, C), BF),
            dma((11,)),
            dma((3,)),
            dma((5,)),
            dma((5,)),
            dma((5,)),
            dma((5,)),
        ],
        compiler_params=pltpu.CompilerParams(collective_id=0, has_side_effects=True),
        name="halo_conv",
    )(
        image, tissue, k1.reshape(9 * C, C), b1.reshape(1, C), k2.reshape(9 * C, C), b2.reshape(1, C)
    )


def solution(mesh):
    in_specs = (P(("slides", "rows"), "cols", None), P(("slides", "rows"), "cols"), P(), P(), P(), P())
    return jax.shard_map(
        shards, mesh=mesh, in_specs=in_specs, out_specs=P(("slides", "rows"), "cols", None), check_vma=False
    )
```

```python
import jax
import jax.numpy as jnp
from jax import lax
from jax.experimental import pallas as pl
from jax.experimental.pallas import tpu as pltpu
from jax.sharding import PartitionSpec as P

MESH = pl.DeviceIdType.MESH
MB = 32
BF = jnp.bfloat16
F32 = jnp.float32
UP, DOWN, SIDE, DUP, DDN = range(5)


def spread(fb, slot, value, r, center, minus, plus):
    W = value.shape[0]
    f = fb.at[slot]
    f[8 : W + 8] = value
    minus[r] = f[7 : W + 7].astype(BF)
    plus[r] = f[9 : W + 9].astype(BF)
    if center is not None:
        center[r] = value.astype(BF)


def clear_ends(fb):
    n, L, C = fb.shape
    for k in range(n):
        fb[k, 0:8] = jnp.zeros((8, C), F32)
        fb[k, L - 8 : L] = jnp.zeros((8, C), F32)


def lhs(p, refs):
    return jnp.concatenate([ref[2 * p + k] for k in range(4) for ref in refs], axis=1)


def finish(acc, bias, mask):
    W, C = acc.shape
    z = jnp.maximum(acc.reshape(W // MB, MB // 8, 8, C) + bias, 0.0) * mask[:, None]
    return z.reshape(W, C)


def block_mask(t, mk, store):
    H, _, C = mk.shape[1:]
    for j in range(H):
        mk[store, j] = jnp.broadcast_to(t[:, j : j + 1], (8, C))


def dot(pieces, w):
    return jnp.dot(jnp.concatenate(pieces, axis=0), w[...], preferred_element_type=F32)


def interior(
    image, tissue, k1, b1, k2, b2,
    xr, xm, xp, pb, h0, hm, hp, ob, w1, w2, bs, ts, mk,
    col, fb, in_sem, send_x, recv_x, send_t, recv_t, ready,
):
    R, W, C = image.shape
    H = W // MB
    n = lax.axis_size("rows")
    sl, i, c = lax.axis_index("slides"), lax.axis_index("rows"), lax.axis_index("cols")
    has_up, has_down, first_col = i > 0, i < n - 1, c == 0
    edge = pl.multiple_of((W - 16) * (1 - c), 16)

    def load(src, dst, k):
        cp = pltpu.make_async_copy(src, dst, in_sem.at[k])
        cp.start()
        return cp

    l_top = load(image.at[0:2], xr.at[2:4], 0)
    l_bot = load(image.at[R - 2 : R], xr.at[R : R + 2], 1)
    l_col = load(image.at[:, pl.ds(edge, 16), :], col, 2)
    l_tis = load(tissue, ts.at[0], 3)
    l_w1 = [load(k1, w1.at[j * 3 * C : j * 3 * C + 9 * C, j * C : (j + 1) * C], 4 + j) for j in range(2)]
    l_img = load(image.at[2 : R - 2], xr.at[4:R], 6)
    l_b1 = load(b1, bs.at[0], 7)
    l_w2 = [load(k2, w2.at[j * 3 * C : j * 3 * C + 9 * C, j * C : (j + 1) * C], 8 + j) for j in range(2)]
    l_b2 = load(b2, bs.at[1], 10)

    up, down = (sl, i - 1, c), (sl, i + 1, c)
    dup, ddn, side = (sl, i - 1, 1 - c), (sl, i + 1, 1 - c), (sl, i, 1 - c)

    def signal(sem, dev):
        pl.semaphore_signal(sem, inc=1, device_id=dev, device_id_type=MESH)

    barrier = pltpu.get_barrier_semaphore()

    @pl.when(has_up)
    def _():
        signal(barrier, up)
        signal(barrier, dup)

    @pl.when(jnp.logical_not(first_col))
    def _():
        signal(barrier, side)

    @pl.when(jnp.logical_or(has_down, first_col))
    def _():
        pl.semaphore_wait(barrier, 2 * has_down.astype(jnp.int32) + (1 - c))

    def remote(src, dst, sends, recvs, k, dev):
        return pltpu.make_async_remote_copy(
            src_ref=src, dst_ref=dst, send_sem=sends.at[k], recv_sem=recvs.at[k],
            device_id=dev, device_id_type=MESH,
        )

    r_up = remote(xr.at[2:4], xr.at[R + 2 : R + 4], send_x, recv_x, UP, up)
    r_down = remote(xr.at[R : R + 2], xr.at[0:2], send_x, recv_x, DOWN, down)
    r_side = remote(col, pb.at[2 : R + 2], send_x, recv_x, SIDE, side)
    r_dup = remote(col.at[0:2], pb.at[R + 2 : R + 4], send_x, recv_x, DUP, dup)
    r_ddn = remote(col.at[R - 2 : R], pb.at[0:2], send_x, recv_x, DDN, ddn)
    t_side = remote(ts.at[0], ts.at[1], send_t, recv_t, SIDE, side)
    t_down = remote(ts.at[0], ts.at[2], send_t, recv_t, DOWN, down)
    t_up = remote(ts.at[0], ts.at[3], send_t, recv_t, UP, up)
    t_ddn = remote(ts.at[0], ts.at[4], send_t, recv_t, DDN, ddn)
    t_dup = remote(ts.at[0], ts.at[5], send_t, recv_t, DUP, dup)

    @pl.when(has_down)
    def _():
        signal(ready.at[0], down)
        signal(ready.at[1], ddn)

    @pl.when(first_col)
    def _():
        signal(ready.at[2], side)

    l_bot.wait()
    l_col.wait()
    l_tis.wait()

    @pl.when(has_down)
    def _():
        r_down.start()
        r_ddn.start()
        t_down.start()
        t_ddn.start()

    @pl.when(first_col)
    def _():
        r_side.start()
        t_side.start()

    for w in (w1, w2):
        w[9 * C : 12 * C, 0:C] = jnp.zeros((3 * C, C), BF)
        w[0 : 3 * C, C : 2 * C] = jnp.zeros((3 * C, C), BF)

    @pl.when(jnp.logical_not(has_up))
    def _():
        xr[0:2] = jnp.zeros((2, W, C), BF)
        pb[0:2] = jnp.zeros((2, 16, C), BF)
        ts[2] = jnp.zeros((1, H), jnp.int32)
        ts[4] = jnp.zeros((1, H), jnp.int32)

    @pl.when(jnp.logical_not(has_down))
    def _():
        xr[R + 2 : R + 4] = jnp.zeros((2, W, C), BF)
        pb[R + 2 : R + 4] = jnp.zeros((2, 16, C), BF)
        ts[3] = jnp.zeros((1, H), jnp.int32)
        ts[5] = jnp.zeros((1, H), jnp.int32)

    clear_ends(fb)
    block_mask(ts[0].astype(F32), mk, 0)
    for cp in (l_top, l_w1[0], l_w1[1], l_b1, l_b2, l_w2[0], l_w2[1], l_img):
        cp.wait()

    own = mk[0]
    counter = [0]

    def shifts(*args):
        spread(fb, counter[0] % fb.shape[0], *args)
        counter[0] += 1

    def halves(acc, pairs, bias):
        for a, p in enumerate(pairs):
            for j in range(2):
                yield 2 * p + j, finish(acc[a * W : (a + 1) * W, j * C : (j + 1) * C], bias, own)

    last = R // 2
    for r in range(2, R + 2):
        shifts(xr[r].astype(F32), r, None, xm, xp)
    for p in range(1, last, 2):
        pairs = [q for q in (p, p + 1) if q < last]
        for r, value in halves(dot([lhs(q, (xm, xr, xp)) for q in pairs], w1), pairs, bs[0]):
            shifts(value, r, h0, hm, hp)
    for p in range(1, last - 1, 2):
        pairs = [q for q in (p, p + 1) if q < last - 1]
        for r, value in halves(dot([lhs(q, (hm, h0, hp)) for q in pairs], w2), pairs, bs[1]):
            ob[r] = value.astype(BF)

    @pl.when(has_up)
    def _():
        pl.semaphore_wait(ready.at[0], 1)
        pl.semaphore_wait(ready.at[1], 1)
        r_up.start()
        r_dup.start()
        t_up.start()
        t_dup.start()

    @pl.when(jnp.logical_not(first_col))
    def _():
        pl.semaphore_wait(ready.at[2], 1)
        r_side.start()
        t_side.start()

    @pl.when(has_up)
    def _():
        for cp in (r_down, r_ddn, t_down, t_ddn):
            cp.wait_recv()
        for cp in (r_up, r_dup, t_up, t_dup):
            cp.wait_send()

    @pl.when(has_down)
    def _():
        for cp in (r_up, r_dup, t_up, t_dup):
            cp.wait_recv()
        for cp in (r_down, r_ddn, t_down, t_ddn):
            cp.wait_send()

    r_side.wait()
    t_side.wait()


def border(
    xr, xm, xp, pb, h0, hm, hp, ob, w1, w2, bs, ts, mk, out,
    ym, y0, yp, gm, g0, gp, em, e0, ep, am, ap, er, nb, mm, ms, fb, sf, hf, out_sem,
):
    R, W, C = ob.shape
    H = W // MB
    c = lax.axis_index("cols")
    left = c == 0
    near = pl.multiple_of((W - 16) * (1 - c), 16)
    far = pl.multiple_of(16 * c, 16)
    outs = []

    def flush(src, dst):
        cp = pltpu.make_async_copy(src, dst, out_sem.at[len(outs)])
        cp.start()
        outs.append(cp)

    flush(ob.at[2 : R - 2, pl.ds(far, W - 16), :], out.at[2 : R - 2, pl.ds(far, W - 16), :])

    clear_ends(fb)
    block_mask(ts[2].astype(F32), mm, 0)
    block_mask(ts[3].astype(F32), mm, 1)
    near_own = jnp.where(left, mk[0, H - 1], mk[0, 0])
    halves = []
    for own, other in ((0, 1), (2, 4), (3, 5)):
        t, o = ts[own].astype(F32), ts[other].astype(F32)
        first = jnp.where(left, t[:, H - 1 : H], o[:, H - 1 : H])
        second = jnp.where(left, o[:, 0:1], t[:, 0:1])
        k = len(halves)
        ms[k, 0] = jnp.broadcast_to(first, (8, C))
        ms[k, 1] = jnp.broadcast_to(second, (8, C))
        halves.append(k)

    bias1, bias2 = bs[0], bs[1]
    last = R // 2
    edges = (0, last)

    for k, r in enumerate((0, 1, R + 2, R + 3)):
        spread(fb, k, xr[r].astype(F32), k, None, am, ap)
    for r in range(R + 4):
        sf[r, pl.ds(pl.multiple_of(16 * c, 16), 16), :] = xr[r, pl.ds(near, 16), :].astype(F32)
        sf[r, pl.ds(pl.multiple_of(16 * (1 - c), 16), 16), :] = pb[r].astype(F32)
        ym[r] = sf[r, 7:23].astype(BF)
        y0[r] = sf[r, 8:24].astype(BF)
        yp[r] = sf[r, 9:25].astype(BF)

    def x_row(r):
        k = {0: 0, 1: 1, R + 2: 2, R + 3: 3}.get(r)
        return [xm[r], xr[r], xp[r]] if k is None else [am[k], xr[r], ap[k]]

    acc = dot(
        [lhs(p, (ym, y0, yp)) for p in range(last + 1)]
        + [jnp.concatenate([v for k in range(4) for v in x_row(2 * p + k)], axis=1) for p in edges],
        w1,
    )
    base = 16 * (last + 1)
    for a, p in enumerate(edges):
        for j in range(2):
            r = 2 * p + j
            mask = mm[0] if r == 0 else mm[1] if r == R + 1 else mk[0]
            value = finish(acc[base + a * W : base + (a + 1) * W, j * C : (j + 1) * C], bias1, mask)
            spread(fb, 2 * a + j, value, 2 * a + j, e0, em, ep)
    for p in range(last + 1):
        for j in range(2):
            r = 2 * p + j
            mask = ms[1 if r == 0 else 2 if r == R + 1 else 0]
            piece = acc[16 * p : 16 * p + 16, j * C : (j + 1) * C].reshape(2, 8, C)
            hf[r, 8:24] = (jnp.maximum(piece + bias1, 0.0) * mask).reshape(16, C)
            k = {0: 0, 1: 1, R: 2, R + 1: 3}.get(r)
            row = h0.at[r] if k is None else e0.at[k]
            rest = row[pl.ds(near, 16), :].astype(F32)
            hf[r, 0:8] = rest[0:8]
            hf[r, 24:32] = rest[8:16]
            gm[r] = hf[r, 7:23].astype(BF)
            g0[r] = hf[r, 8:24].astype(BF)
            gp[r] = hf[r, 9:25].astype(BF)

    def h_row(r):
        k = {0: 0, 1: 1, R: 2, R + 1: 3}.get(r)
        return [hm[r], h0[r], hp[r]] if k is None else [em[k], e0[k], ep[k]]

    ends = (0, last - 1)
    acc = dot(
        [jnp.concatenate([v for k in range(4) for v in h_row(2 * p + k)], axis=1) for p in ends]
        + [lhs(p, (gm, g0, gp)) for p in range(last)],
        w2,
    )
    for a, p in enumerate(ends):
        for j in range(2):
            er[2 * a + j] = finish(acc[a * W : (a + 1) * W, j * C : (j + 1) * C], bias2, mk[0]).astype(BF)
    flush(er.at[0:2, pl.ds(far, W - 16), :], out.at[0:2, pl.ds(far, W - 16), :])
    flush(er.at[2:4, pl.ds(far, W - 16), :], out.at[R - 2 : R, pl.ds(far, W - 16), :])
    for p in range(last):
        for j in range(2):
            r = 2 * p + j
            lo = 2 * W + 16 * p
            piece = acc[lo : lo + 16, j * C : (j + 1) * C].reshape(2, 8, C)
            new = jnp.maximum(jnp.where(left, piece[0], piece[1]) + bias2, 0.0) * near_own
            k = {0: 0, 1: 1, R - 2: 2, R - 1: 3}.get(r)
            row = ob.at[r] if k is None else er.at[k]
            old = row[pl.ds(near, 16), :].astype(F32)
            first = jnp.where(left, old[0:8], new)
            second = jnp.where(left, new, old[8:16])
            nb[r] = jnp.concatenate([first, second], axis=0).astype(BF)
    flush(nb, out.at[:, pl.ds(near, 16), :])
    for cp in outs:
        cp.wait()


def shards(image, tissue, k1, b1, k2, b2):
    R, W, C = image.shape
    H = W // MB
    any_spec = pl.BlockSpec(memory_space=pl.ANY)
    vmem = pl.BlockSpec(memory_space=pltpu.VMEM)
    hbm = pl.BlockSpec(memory_space=pltpu.HBM)
    dma = pltpu.SemaphoreType.DMA
    passed = [
        ((R + 4, W, C), BF), ((R + 4, W, C), BF), ((R + 4, W, C), BF), ((R + 4, 16, C), BF),
        ((R + 2, W, C), BF), ((R + 2, W, C), BF), ((R + 2, W, C), BF), ((R, W, C), BF),
        ((12 * C, 2 * C), BF), ((12 * C, 2 * C), BF), ((2, 1, C), F32), ((6, 1, H), jnp.int32),
        ((1, H, 8, C), F32),
    ]
    state = pl.pallas_call(
        interior,
        out_shape=[jax.ShapeDtypeStruct(*s) for s in passed],
        in_specs=[hbm] * 6,
        out_specs=[vmem] * len(passed),
        scratch_shapes=[
            pltpu.VMEM((R, 16, C), BF),
            pltpu.VMEM((4, W + 16, C), F32),
            dma((11,)), dma((5,)), dma((5,)), dma((5,)), dma((5,)),
            pltpu.SemaphoreType.REGULAR((3,)),
        ],
        compiler_params=pltpu.CompilerParams(
            collective_id=0, has_side_effects=True, vmem_limit_bytes=24 * 1024 * 1024
        ),
        name="interior",
    )(
        *(
            pltpu.with_memory_space_constraint(v, pltpu.HBM)
            for v in (
                image, tissue, k1.reshape(9 * C, C), b1.reshape(1, C), k2.reshape(9 * C, C), b2.reshape(1, C)
            )
        )
    )
    window = lambda rows, dtype=BF, px=16: pltpu.VMEM((rows, px, C), dtype)
    row = lambda rows: pltpu.VMEM((rows, W, C), BF)
    return pl.pallas_call(
        border,
        out_shape=jax.ShapeDtypeStruct((R, W, C), BF),
        in_specs=[vmem] * len(passed),
        out_specs=any_spec,
        scratch_shapes=[
            window(R + 4), window(R + 4), window(R + 4), window(R + 2), window(R + 2), window(R + 2),
            row(4), row(4), row(4), row(4), row(4), row(4), window(R),
            pltpu.VMEM((2, H, 8, C), F32), pltpu.VMEM((3, 2, 8, C), F32),
            pltpu.VMEM((4, W + 16, C), F32), window(R + 4, F32, 32), window(R + 2, F32, 32),
            dma((4,)),
        ],
        compiler_params=pltpu.CompilerParams(vmem_limit_bytes=24 * 1024 * 1024),
        name="border",
    )(*state)


def solution(mesh):
    in_specs = (P(("slides", "rows"), "cols", None), P(("slides", "rows"), "cols"), P(), P(), P(), P())
    return jax.shard_map(
        shards, mesh=mesh, in_specs=in_specs, out_specs=P(("slides", "rows"), "cols", None), check_vma=False
    )
```

```python
import jax
import jax.numpy as jnp
from jax import lax
from jax.experimental import pallas as pl
from jax.experimental.pallas import tpu as pltpu
from jax.sharding import PartitionSpec as P

MESH = pl.DeviceIdType.MESH
MB = 32
BF = jnp.bfloat16
F32 = jnp.float32
UP, DOWN, SIDE, DUP, DDN = range(5)


def spread(fb, slot, value, r, center, minus, plus, window=None):
    W = value.shape[0]
    f = fb.at[slot]
    f[8 : W + 8] = value
    if window is not None:
        f[pl.ds(pl.multiple_of(W * (1 - lax.axis_index("cols")), 8), 16), :] = window
        value = f[8 : W + 8]
    minus[r] = f[7 : W + 7].astype(BF)
    plus[r] = f[9 : W + 9].astype(BF)
    if center is not None:
        center[r] = value.astype(BF)


def windows(xr, pb, sf, r, ym, y0, yp):
    W = xr.shape[1]
    c = lax.axis_index("cols")
    near = pl.multiple_of((W - 16) * (1 - c), 16)
    sf[r, pl.ds(pl.multiple_of(16 * c, 16), 16), :] = xr[r, pl.ds(near, 16), :].astype(F32)
    sf[r, pl.ds(pl.multiple_of(16 * (1 - c), 16), 16), :] = pb[r].astype(F32)
    ym[r] = sf[r, 7:23].astype(BF)
    y0[r] = sf[r, 8:24].astype(BF)
    yp[r] = sf[r, 9:25].astype(BF)


def window_mask(ts, ms, k, own, other):
    H, C = ts.shape[2], ms.shape[3]
    left = lax.axis_index("cols") == 0
    t, o = ts[own].astype(F32), ts[other].astype(F32)
    first = jnp.where(left, t[:, H - 1 : H], o[:, H - 1 : H])
    second = jnp.where(left, o[:, 0:1], t[:, 0:1])
    ms[k, 0] = jnp.broadcast_to(first, (8, C))
    ms[k, 1] = jnp.broadcast_to(second, (8, C))


def window_finish(piece, bias, mask):
    C = piece.shape[1]
    return (jnp.maximum(piece.reshape(2, 8, C) + bias, 0.0) * mask).reshape(16, C)


def clear_ends(fb):
    n, L, C = fb.shape
    for k in range(n):
        fb[k, 0:8] = jnp.zeros((8, C), F32)
        fb[k, L - 8 : L] = jnp.zeros((8, C), F32)


def wide(pieces):
    return jnp.concatenate(pieces, axis=1)


def lhs(p, refs):
    return wide([ref[2 * p + k] for k in range(4) for ref in refs])


def finish(acc, bias, mask):
    W, C = acc.shape
    z = jnp.maximum(acc.reshape(W // MB, MB // 8, 8, C) + bias, 0.0) * mask[:, None]
    return z.reshape(W, C)


def block_mask(t, mk, store):
    H, _, C = mk.shape[1:]
    for j in range(H):
        mk[store, j] = jnp.broadcast_to(t[:, j : j + 1], (8, C))


def dot(pieces, w):
    return jnp.dot(jnp.concatenate(pieces, axis=0), w[...], preferred_element_type=F32)


def interior(
    image, tissue, k1, b1, k2, b2,
    xr, xm, xp, pb, h0, hm, hp, ob, w1, w2, bs, ts, mk,
    col, fb, sf, hf, ym, y0, yp, gm, g0, gp, ms, in_sem, send_x, recv_x, send_t, recv_t, ready,
):
    R, W, C = image.shape
    H = W // MB
    n = lax.axis_size("rows")
    sl, i, c = lax.axis_index("slides"), lax.axis_index("rows"), lax.axis_index("cols")
    has_up, has_down, first_col = i > 0, i < n - 1, c == 0
    edge = pl.multiple_of((W - 16) * (1 - c), 16)

    def load(src, dst, k):
        cp = pltpu.make_async_copy(src, dst, in_sem.at[k])
        cp.start()
        return cp

    l_top = load(image.at[0:2], xr.at[2:4], 0)
    l_bot = load(image.at[R - 2 : R], xr.at[R : R + 2], 1)
    l_col = load(image.at[:, pl.ds(edge, 16), :], col, 2)
    l_tis = load(tissue, ts.at[0], 3)
    l_w1 = [load(k1, w1.at[j * 3 * C : j * 3 * C + 9 * C, j * C : (j + 1) * C], 4 + j) for j in range(2)]
    l_img = load(image.at[2 : R - 2], xr.at[4:R], 6)
    l_b1 = load(b1, bs.at[0], 7)
    l_w2 = [load(k2, w2.at[j * 3 * C : j * 3 * C + 9 * C, j * C : (j + 1) * C], 8 + j) for j in range(2)]
    l_b2 = load(b2, bs.at[1], 10)

    up, down = (sl, i - 1, c), (sl, i + 1, c)
    dup, ddn, side = (sl, i - 1, 1 - c), (sl, i + 1, 1 - c), (sl, i, 1 - c)

    def signal(sem, dev):
        pl.semaphore_signal(sem, inc=1, device_id=dev, device_id_type=MESH)

    barrier = pltpu.get_barrier_semaphore()

    @pl.when(has_up)
    def _():
        signal(barrier, up)
        signal(barrier, dup)

    @pl.when(jnp.logical_not(first_col))
    def _():
        signal(barrier, side)

    @pl.when(jnp.logical_or(has_down, first_col))
    def _():
        pl.semaphore_wait(barrier, 2 * has_down.astype(jnp.int32) + (1 - c))

    def remote(src, dst, sends, recvs, k, dev):
        return pltpu.make_async_remote_copy(
            src_ref=src, dst_ref=dst, send_sem=sends.at[k], recv_sem=recvs.at[k],
            device_id=dev, device_id_type=MESH,
        )

    r_up = remote(xr.at[2:4], xr.at[R + 2 : R + 4], send_x, recv_x, UP, up)
    r_down = remote(xr.at[R : R + 2], xr.at[0:2], send_x, recv_x, DOWN, down)
    r_side = remote(col, pb.at[2 : R + 2], send_x, recv_x, SIDE, side)
    r_dup = remote(col.at[0:2], pb.at[R + 2 : R + 4], send_x, recv_x, DUP, dup)
    r_ddn = remote(col.at[R - 2 : R], pb.at[0:2], send_x, recv_x, DDN, ddn)
    t_side = remote(ts.at[0], ts.at[1], send_t, recv_t, SIDE, side)
    t_down = remote(ts.at[0], ts.at[2], send_t, recv_t, DOWN, down)
    t_up = remote(ts.at[0], ts.at[3], send_t, recv_t, UP, up)
    t_ddn = remote(ts.at[0], ts.at[4], send_t, recv_t, DDN, ddn)
    t_dup = remote(ts.at[0], ts.at[5], send_t, recv_t, DUP, dup)

    @pl.when(has_down)
    def _():
        signal(ready.at[0], down)
        signal(ready.at[1], ddn)

    @pl.when(first_col)
    def _():
        signal(ready.at[2], side)

    l_bot.wait()
    l_col.wait()
    l_tis.wait()

    @pl.when(has_down)
    def _():
        r_down.start()
        r_ddn.start()
        t_down.start()
        t_ddn.start()

    @pl.when(first_col)
    def _():
        r_side.start()
        t_side.start()

    for w in (w1, w2):
        w[9 * C : 12 * C, 0:C] = jnp.zeros((3 * C, C), BF)
        w[0 : 3 * C, C : 2 * C] = jnp.zeros((3 * C, C), BF)

    @pl.when(jnp.logical_not(has_up))
    def _():
        xr[0:2] = jnp.zeros((2, W, C), BF)
        pb[0:2] = jnp.zeros((2, 16, C), BF)
        ts[2] = jnp.zeros((1, H), jnp.int32)
        ts[4] = jnp.zeros((1, H), jnp.int32)

    @pl.when(jnp.logical_not(has_down))
    def _():
        xr[R + 2 : R + 4] = jnp.zeros((2, W, C), BF)
        pb[R + 2 : R + 4] = jnp.zeros((2, 16, C), BF)
        ts[3] = jnp.zeros((1, H), jnp.int32)
        ts[5] = jnp.zeros((1, H), jnp.int32)

    clear_ends(fb)
    block_mask(ts[0].astype(F32), mk, 0)
    for cp in (l_top, l_w1[0], l_w1[1], l_b1, l_b2, l_w2[0], l_w2[1], l_img):
        cp.wait()

    own = mk[0]
    counter = [0]

    def shifts(*args):
        spread(fb, counter[0] % fb.shape[0], *args)
        counter[0] += 1

    def halves(acc, pairs, bias):
        for a, p in enumerate(pairs):
            for j in range(2):
                yield 2 * p + j, finish(acc[a * W : (a + 1) * W, j * C : (j + 1) * C], bias, own)

    last = R // 2
    for r in range(2, R + 2):
        shifts(xr[r].astype(F32), r, None, xm, xp)
    for p in range(1, last, 2):
        pairs = [q for q in (p, p + 1) if q < last]
        for r, value in halves(dot([lhs(q, (xm, xr, xp)) for q in pairs], w1), pairs, bs[0]):
            shifts(value, r, h0, hm, hp)
    for p in range(1, last - 1, 2):
        pairs = [q for q in (p, p + 1) if q < last - 1]
        for r, value in halves(dot([lhs(q, (hm, h0, hp)) for q in pairs], w2), pairs, bs[1]):
            ob[r] = value.astype(BF)

    @pl.when(jnp.logical_and(has_up, first_col))
    def _():
        pl.semaphore_wait(ready.at[1], 1)
        r_dup.start()
        t_dup.start()

    @pl.when(jnp.logical_and(has_up, jnp.logical_not(first_col)))
    def _():
        pl.semaphore_wait(ready.at[0], 1)
        r_up.start()
        t_up.start()

    @pl.when(jnp.logical_not(first_col))
    def _():
        pl.semaphore_wait(ready.at[2], 1)
        r_side.start()
        t_side.start()

    @pl.when(jnp.logical_and(has_up, first_col))
    def _():
        pl.semaphore_wait(ready.at[0], 1)
        r_up.start()
        t_up.start()

    @pl.when(jnp.logical_and(has_up, jnp.logical_not(first_col)))
    def _():
        pl.semaphore_wait(ready.at[1], 1)
        r_dup.start()
        t_dup.start()

    r_side.wait_recv()
    t_side.wait_recv()

    @pl.when(has_down)
    def _():
        for cp in (r_up, r_dup, t_up, t_dup):
            cp.wait_recv()

    block_mask(ts[3].astype(F32), mk, 1)
    window_mask(ts, ms, 0, 0, 1)
    window_mask(ts, ms, 1, 3, 5)
    near_own = jnp.where(first_col, own[H - 1], own[0])
    for r in range(2, R + 4):
        windows(xr, pb, sf, r, ym, y0, yp)
    for r in (R, R + 1, R + 2, R + 3, 2, 3):
        shifts(xr[r].astype(F32), r, None, xm, xp, sf[r, 8:24])
    acc = dot([lhs(p, (ym, y0, yp)) for p in range(1, last + 1)] + [lhs(last, (xm, xr, xp))], w1)
    for p in range(1, last + 1):
        for j in range(2):
            r = 2 * p + j
            piece = acc[16 * p - 16 : 16 * p, j * C : (j + 1) * C]
            hf[r, 8:24] = window_finish(piece, bs[0], ms[1 if r == R + 1 else 0])
            if r < R:
                rest = h0[r, pl.ds(edge, 16), :].astype(F32)
                hf[r, 0:8] = rest[0:8]
                hf[r, 24:32] = rest[8:16]
                gm[r] = hf[r, 7:23].astype(BF)
                g0[r] = hf[r, 8:24].astype(BF)
                gp[r] = hf[r, 9:25].astype(BF)
    for r in (R - 2, R - 1, 2, 3):
        shifts(h0[r].astype(F32), r, h0, hm, hp, hf[r, 8:24])
    for j in range(2):
        r = R + j
        value = finish(acc[16 * last : 16 * last + W, j * C : (j + 1) * C], bs[0], mk[j])
        shifts(value, r, h0, hm, hp, hf[r, 8:24])
    acc = dot([lhs(p, (gm, g0, gp)) for p in range(1, last - 1)] + [lhs(last - 1, (hm, h0, hp))], w2)
    for p in range(1, last - 1):
        for j in range(2):
            piece = acc[16 * p - 16 : 16 * p, j * C : (j + 1) * C].reshape(2, 8, C)
            new = jnp.maximum(jnp.where(first_col, piece[0], piece[1]) + bs[1], 0.0) * near_own
            ob[2 * p + j, pl.ds(pl.multiple_of((W - 8) * (1 - c), 8), 8), :] = new.astype(BF)
    for j in range(2):
        lo = 16 * (last - 2)
        ob[R - 2 + j] = finish(acc[lo : lo + W, j * C : (j + 1) * C], bs[1], own).astype(BF)

    r_side.wait_send()
    t_side.wait_send()

    @pl.when(has_down)
    def _():
        for cp in (r_down, r_ddn, t_down, t_ddn):
            cp.wait_send()

    @pl.when(has_up)
    def _():
        for cp in (r_down, r_ddn, t_down, t_ddn):
            cp.wait_recv()
        for cp in (r_up, r_dup, t_up, t_dup):
            cp.wait_send()


def top(
    xr, xm, xp, pb, h0, hm, hp, ob, w1, w2, bs, ts, mk, out,
    ym, y0, yp, am, ap, em, e0, ep, er, mm, ms, fb, sf, out_sem,
):
    R, W, C = ob.shape
    rest = pltpu.make_async_copy(ob.at[2:R], out.at[2:R], out_sem.at[0])
    rest.start()
    clear_ends(fb)
    block_mask(ts[2].astype(F32), mm, 0)
    window_mask(ts, ms, 0, 2, 4)
    window_mask(ts, ms, 1, 0, 1)
    for r in range(4):
        windows(xr, pb, sf, r, ym, y0, yp)
    for r in range(2):
        spread(fb, r, xr[r].astype(F32), r, None, am, ap, sf[r, 8:24])
    rows = [(am, xr, ap), (am, xr, ap), (xm, xr, xp), (xm, xr, xp)]
    acc = dot([lhs(0, (ym, y0, yp)), wide([ref[k] for k in range(4) for ref in rows[k]])], w1)
    for j in range(2):
        part = acc[:, j * C : (j + 1) * C]
        window = window_finish(part[0:16], bs[0], ms[j])
        spread(fb, 2 + j, finish(part[16 : 16 + W], bs[0], mk[0] if j else mm[0]), j, e0, em, ep, window)
    rows = [(em, e0, ep), (em, e0, ep), (hm, h0, hp), (hm, h0, hp)]
    acc = dot([wide([ref[k] for k in range(4) for ref in rows[k]])], w2)
    for j in range(2):
        er[j] = finish(acc[:, j * C : (j + 1) * C], bs[1], mk[0]).astype(BF)
    first = pltpu.make_async_copy(er, out.at[0:2], out_sem.at[1])
    first.start()
    rest.wait()
    first.wait()


def shards(image, tissue, k1, b1, k2, b2):
    R, W, C = image.shape
    H = W // MB
    any_spec = pl.BlockSpec(memory_space=pl.ANY)
    vmem = pl.BlockSpec(memory_space=pltpu.VMEM)
    hbm = pl.BlockSpec(memory_space=pltpu.HBM)
    dma = pltpu.SemaphoreType.DMA
    passed = [
        ((R + 4, W, C), BF), ((R + 4, W, C), BF), ((R + 4, W, C), BF), ((R + 4, 16, C), BF),
        ((R + 2, W, C), BF), ((R + 2, W, C), BF), ((R + 2, W, C), BF), ((R, W, C), BF),
        ((12 * C, 2 * C), BF), ((12 * C, 2 * C), BF), ((2, 1, C), F32), ((6, 1, H), jnp.int32),
        ((2, H, 8, C), F32),
    ]
    window = lambda rows, dtype=BF, px=16: pltpu.VMEM((rows, px, C), dtype)
    row = lambda rows: pltpu.VMEM((rows, W, C), BF)
    state = pl.pallas_call(
        interior,
        out_shape=[jax.ShapeDtypeStruct(*s) for s in passed],
        in_specs=[hbm] * 6,
        out_specs=[vmem] * len(passed),
        scratch_shapes=[
            window(R),
            pltpu.VMEM((4, W + 16, C), F32), window(R + 4, F32, 32), window(R + 2, F32, 32),
            window(R + 4), window(R + 4), window(R + 4), window(R + 2), window(R + 2), window(R + 2),
            pltpu.VMEM((2, 2, 8, C), F32),
            dma((11,)), dma((5,)), dma((5,)), dma((5,)), dma((5,)),
            pltpu.SemaphoreType.REGULAR((3,)),
        ],
        compiler_params=pltpu.CompilerParams(
            collective_id=0, has_side_effects=True, vmem_limit_bytes=24 * 1024 * 1024
        ),
        name="interior",
    )(
        *(
            pltpu.with_memory_space_constraint(v, pltpu.HBM)
            for v in (
                image, tissue, k1.reshape(9 * C, C), b1.reshape(1, C), k2.reshape(9 * C, C), b2.reshape(1, C)
            )
        )
    )
    return pl.pallas_call(
        top,
        out_shape=jax.ShapeDtypeStruct((R, W, C), BF),
        in_specs=[vmem] * len(passed),
        out_specs=any_spec,
        scratch_shapes=[
            window(4), window(4), window(4),
            row(2), row(2), row(2), row(2), row(2), row(2),
            pltpu.VMEM((1, H, 8, C), F32), pltpu.VMEM((2, 2, 8, C), F32),
            pltpu.VMEM((4, W + 16, C), F32), window(4, F32, 32),
            dma((2,)),
        ],
        compiler_params=pltpu.CompilerParams(vmem_limit_bytes=24 * 1024 * 1024),
        name="border",
    )(*state)


def solution(mesh):
    in_specs = (P(("slides", "rows"), "cols", None), P(("slides", "rows"), "cols"), P(), P(), P(), P())
    return jax.shard_map(
        shards, mesh=mesh, in_specs=in_specs, out_specs=P(("slides", "rows"), "cols", None), check_vma=False
    )
```
